32 devices in a mesh: section: 8 (over z, x), dp: 4 (over y, core).
Axes of the slice: x: 2, y: 2, z: 4, core: 2. Of those that a mesh axis runs over, the one named last changes fastest.
Arguments:
- carry_act: bfloat16 [8, 32, 2304], P('section', 'dp'), may hold values from -6 to 6
- carry_act_tan: bfloat16 [8, 32, 2304], P('section', 'dp'), may hold values from -6 to 6
- carry_adj: bfloat16 [8, 32, 2304], P('section', 'dp'), may hold values from -0.75 to 0.75
- carry_adj_tan: bfloat16 [8, 32, 2304], P('section', 'dp'), may hold values from -0.75 to 0.75
- fresh_act: bfloat16 [2, 32, 2304], P(None, 'dp'), may hold values from -6 to 6
- loss_cot: bfloat16 [2, 32, 2304], P(None, 'dp'), may hold values from -0.75 to 0.75
- stash_act: bfloat16 [8, 2, 32, 2304], P('section', None, 'dp'), may hold values from -6 to 6
- stash_act_tan: bfloat16 [8, 2, 32, 2304], P('section', None, 'dp'), may hold values from -6 to 6
- norm_gain: bfloat16 [8, 2304], P('section'), may hold values from 0.25 to 1.75
- up_weight: bfloat16 [8, 2304, 4608], P('section', None, 'dp'), may hold values from -0.125 to 0.125
- down_weight: bfloat16 [8, 4608, 2304], P('section', 'dp'), may hold values from -0.09375 to 0.09375
- up_dir: bfloat16 [8, 2304, 4608], P('section', None, 'dp'), may hold values from -0.125 to 0.125
- down_dir: bfloat16 [8, 4608, 2304], P('section', 'dp'), may hold values from -0.09375 to 0.09375
Outputs:
- next_act: bfloat16 [8, 32, 2304], P('section', 'dp')
- next_act_tan: bfloat16 [8, 32, 2304], P('section', 'dp')
- next_adj: bfloat16 [8, 32, 2304], P('section', 'dp')
- next_adj_tan: bfloat16 [8, 32, 2304], P('section', 'dp')
- hvp_up: bfloat16 [8, 2304, 4608], P('section', None, 'dp')
- hvp_down: bfloat16 [8, 4608, 2304], P('section', 'dp')
The draws below stay inside these ranges and needn't reach their ends.
All inputs are finite; a program needn't handle non-finite values.
Results may differ from the reference program's by a relative error of at most 0.02.
Values may be sent and summed in bfloat16 or wider, within the bound.
A program may use at most 128 MiB of HBM per device.

```python
import jax
import jax.numpy as jnp
from jax import lax

D = 2304
FF = 4608
TICKS = 2
TOKENS = 32
SECTIONS = 8
N_DP = 4


def block_levels(key, dims, split, low, top_value):
    factor_of = 1.0
    for position, blocks in split:
        draws = jax.random.uniform(jax.random.fold_in(jax.random.fold_in(key, 6), position), (blocks,), jnp.float32, low / len(split), top_value / len(split))
        factor_of = factor_of * jnp.repeat(jnp.exp(draws), dims[position] // blocks).reshape((-1,) + (1,) * (len(dims) - 1 - position))
    return factor_of


def noise(own_key, dims, scale, reach, cuts=(), dtype=jnp.bfloat16):
    entries = scale * jax.random.normal(own_key, dims, jnp.float32)
    if cuts:
        entries = entries * block_levels(own_key, dims, cuts, -0.22, 0.18)
    return jnp.clip(entries, -reach, reach).astype(dtype)


def setup_inputs(seed: int = 0) -> dict:
    splits = jax.random.split(jax.random.key(seed), 14)
    carry_act = noise(splits[0], (SECTIONS, TOKENS, D), 1.0, 6.0, ((0, 8), (1, 4)))
    carry_act_tan = noise(splits[1], (SECTIONS, TOKENS, D), 1.0, 6.0, ((0, 8), (1, 4)))
    carry_adj = noise(splits[2], (SECTIONS, TOKENS, D), 0.125, 0.75, ((0, 8), (1, 4)))
    carry_adj_tan = noise(splits[3], (SECTIONS, TOKENS, D), 0.125, 0.75, ((0, 8), (1, 4)))
    fresh_act = noise(splits[4], (TICKS, TOKENS, D), 1.0, 6.0, ((1, 4),))
    loss_cot = noise(splits[5], (TICKS, TOKENS, D), 0.125, 0.75, ((1, 4),))
    stash_act = noise(splits[6], (SECTIONS, TICKS, TOKENS, D), 1.0, 6.0, ((0, 8), (2, 4)))
    stash_act_tan = noise(splits[7], (SECTIONS, TICKS, TOKENS, D), 1.0, 6.0, ((0, 8), (2, 4)))
    norm_gain = jnp.clip(1.0 + 0.15 * jax.random.normal(splits[8], (SECTIONS, D), jnp.float32), 0.25, 1.75).astype(jnp.bfloat16)
    up_weight = noise(splits[9], (SECTIONS, D, FF), D ** -0.5, 0.125, ((0, 8), (2, 4)))
    down_weight = noise(splits[10], (SECTIONS, FF, D), FF ** -0.5, 0.09375, ((0, 8), (1, 4)))
    up_dir = noise(splits[11], (SECTIONS, D, FF), D ** -0.5, 0.125, ((0, 8), (2, 4)))
    down_dir = noise(splits[12], (SECTIONS, FF, D), FF ** -0.5, 0.09375, ((0, 8), (1, 4)))
    return dict(carry_act=carry_act, carry_act_tan=carry_act_tan, carry_adj=carry_adj, carry_adj_tan=carry_adj_tan, fresh_act=fresh_act, loss_cot=loss_cot, stash_act=stash_act, stash_act_tan=stash_act_tan, norm_gain=norm_gain, up_weight=up_weight, down_weight=down_weight, up_dir=up_dir, down_dir=down_dir)


sqrt_two_over_pi = 0.7978845608028654
cubic_coef = 0.044715
norm_eps = 1e-06

def gelu_parts(linear):
    inner_arg = sqrt_two_over_pi * (linear + cubic_coef * linear * linear * linear)
    first_slope = sqrt_two_over_pi * (1.0 + 3.0 * cubic_coef * linear * linear)
    second_slope = 6.0 * sqrt_two_over_pi * cubic_coef * linear
    tanh_value = jnp.tanh(inner_arg)
    sech_square = 1.0 - tanh_value * tanh_value
    gelu_value = 0.5 * linear * (1.0 + tanh_value)
    gelu_first = 0.5 * (1.0 + tanh_value) + 0.5 * linear * sech_square * first_slope
    gelu_second = sech_square * (first_slope - linear * tanh_value * first_slope * first_slope + 0.5 * linear * second_slope)
    return (gelu_value, gelu_first, gelu_second)

def matrix_product(left, right):
    return jnp.dot(left, right, preferred_element_type=jnp.float32)

def product_last(left, right):
    return lax.dot_general(left, right, (((1,), (1,)), ((), ())), preferred_element_type=jnp.float32)

def product_first(left, right):
    return lax.dot_general(left, right, (((0,), (0,)), ((), ())), preferred_element_type=jnp.float32)

def norm_stats(rows, rows_tan):
    values = rows.astype(jnp.float32)
    values_tan = rows_tan.astype(jnp.float32)
    inverse = lax.rsqrt(lax.optimization_barrier(jnp.mean(values * values, axis=-1, keepdims=True)) + norm_eps)
    inverse_tan = -(inverse * inverse * inverse) * lax.optimization_barrier(jnp.mean(values * values_tan, axis=-1, keepdims=True))
    return (values, values_tan, inverse, inverse_tan)

def norm_rows(rows, rows_tan, gain_row):
    values, values_tan, inverse, inverse_tan = norm_stats(rows, rows_tan)
    gain_wide = gain_row.astype(jnp.float32)
    normed = (values * inverse * gain_wide).astype(jnp.bfloat16)
    normed_tan = ((values_tan * inverse + values * inverse_tan) * gain_wide).astype(jnp.bfloat16)
    return (normed, normed_tan)

def norm_back(rows, rows_tan, gain_row, arriving, arriving_tan, summed, summed_tan):
    values, values_tan, inverse, inverse_tan = norm_stats(rows, rows_tan)
    gain_wide = gain_row.astype(jnp.float32)
    weighted = summed * gain_wide
    weighted_tan = summed_tan * gain_wide
    moment = lax.optimization_barrier(jnp.mean(values * weighted, axis=-1, keepdims=True))
    moment_tan = lax.optimization_barrier(jnp.mean(values_tan * weighted + values * weighted_tan, axis=-1, keepdims=True))
    inverse_cube = inverse * inverse * inverse
    returned = arriving.astype(jnp.float32) + inverse * weighted - inverse_cube * values * moment
    returned_tan = arriving_tan.astype(jnp.float32) + inverse_tan * weighted + inverse * weighted_tan - 3.0 * inverse * inverse * inverse_tan * values * moment - inverse_cube * values_tan * moment - inverse_cube * values * moment_tan
    return (returned.astype(jnp.bfloat16), returned_tan.astype(jnp.bfloat16))

def branch_forward(normed, normed_tan, up_local, down_local, up_direction, down_direction):
    linear = matrix_product(normed, up_local)
    linear_tan = matrix_product(normed_tan, up_local) + matrix_product(normed, up_direction)
    gelu_value, gelu_first, gelu_second = gelu_parts(linear)
    hidden = gelu_value.astype(jnp.bfloat16)
    hidden_tan = (gelu_first * linear_tan).astype(jnp.bfloat16)
    partial_value = matrix_product(hidden, down_local)
    partial_tan = matrix_product(hidden_tan, down_local) + matrix_product(hidden, down_direction)
    return (partial_value, partial_tan)

def branch_backward(stash_normed, stash_normed_tan, adjoint_all, adjoint_all_tan, up_local, down_local, up_direction, down_direction):
    linear = matrix_product(stash_normed, up_local)
    linear_tan = matrix_product(stash_normed_tan, up_local) + matrix_product(stash_normed, up_direction)
    gelu_value, gelu_first, gelu_second = gelu_parts(linear)
    hidden = gelu_value.astype(jnp.bfloat16)
    hidden_tan = (gelu_first * linear_tan).astype(jnp.bfloat16)
    upstream = product_last(adjoint_all, down_local)
    upstream_tan = product_last(adjoint_all_tan, down_local) + product_last(adjoint_all, down_direction)
    deltas = (upstream * gelu_first).astype(jnp.bfloat16)
    deltas_tan = (upstream_tan * gelu_first + upstream * gelu_second * linear_tan).astype(jnp.bfloat16)
    curvature_down = product_first(hidden_tan, adjoint_all) + product_first(hidden, adjoint_all_tan)
    curvature_up = product_first(stash_normed_tan, deltas) + product_first(stash_normed, deltas_tan)
    partial_value = product_last(deltas, up_local)
    partial_tan = product_last(deltas_tan, up_local) + product_last(deltas, up_direction)
    return (partial_value, partial_tan, curvature_up, curvature_down)

def sum_slices(parts):
    rounded = lax.optimization_barrier(parts.astype(jnp.bfloat16)).astype(jnp.float32)
    return lax.optimization_barrier(jnp.sum(rounded, axis=0))

def one_section(packed):
    input_rows, input_tan, arriving, arriving_tan, stash_rows, stash_tan, gain_row, up_section, down_section, up_section_dir, down_section_dir = packed
    width = FF // N_DP
    up_sliced = jnp.moveaxis(up_section.reshape(D, N_DP, width), 1, 0)
    up_dir_sliced = jnp.moveaxis(up_section_dir.reshape(D, N_DP, width), 1, 0)
    down_sliced = down_section.reshape(N_DP, width, D)
    down_dir_sliced = down_section_dir.reshape(N_DP, width, D)
    normed, normed_tan = norm_rows(input_rows, input_tan, gain_row)

    def forward_slice(weights):
        return branch_forward(normed, normed_tan, weights[0], weights[1], weights[2], weights[3])
    partials = lax.map(forward_slice, (up_sliced, down_sliced, up_dir_sliced, down_dir_sliced))
    new_act = (input_rows.astype(jnp.float32) + sum_slices(partials[0])).astype(jnp.bfloat16)
    new_act_tan = (input_tan.astype(jnp.float32) + sum_slices(partials[1])).astype(jnp.bfloat16)
    stash_normed, stash_normed_tan = norm_rows(stash_rows, stash_tan, gain_row)

    def backward_slice(weights):
        return branch_backward(stash_normed, stash_normed_tan, arriving, arriving_tan, weights[0], weights[1], weights[2], weights[3])
    backs = lax.map(backward_slice, (up_sliced, down_sliced, up_dir_sliced, down_dir_sliced))
    summed = sum_slices(backs[0])
    summed_tan = sum_slices(backs[1])
    curvature_up = jnp.moveaxis(backs[2], 0, 1).reshape(D, FF)
    curvature_down = backs[3].reshape(FF, D)
    new_adj, new_adj_tan = norm_back(stash_rows, stash_tan, gain_row, arriving, arriving_tan, summed, summed_tan)
    return (new_act, new_act_tan, new_adj, new_adj_tan, curvature_up, curvature_down)

def reference(carry_act, carry_act_tan, carry_adj, carry_adj_tan, fresh_act, loss_cot, stash_act, stash_act_tan, norm_gain, up_weight, down_weight, up_dir, down_dir):
    activation, activation_tan = (carry_act, carry_act_tan)
    adjoint, adjoint_tan = (carry_adj, carry_adj_tan)
    total_up = jnp.zeros(up_weight.shape, jnp.float32)
    total_down = jnp.zeros(down_weight.shape, jnp.float32)
    for tick_index in range(TICKS):
        zero_rows = jnp.zeros_like(fresh_act[tick_index])
        input_rows = jnp.concatenate([fresh_act[tick_index][None], activation[:-1]], axis=0)
        input_tan = jnp.concatenate([zero_rows[None], activation_tan[:-1]], axis=0)
        arriving = jnp.concatenate([adjoint[1:], loss_cot[tick_index][None]], axis=0)
        arriving_tan = jnp.concatenate([adjoint_tan[1:], zero_rows[None]], axis=0)
        results = lax.map(one_section, (input_rows, input_tan, arriving, arriving_tan, stash_act[:, tick_index], stash_act_tan[:, tick_index], norm_gain, up_weight, down_weight, up_dir, down_dir))
        activation, activation_tan, adjoint, adjoint_tan = (results[0], results[1], results[2], results[3])
        total_up = total_up + results[4]
        total_down = total_down + results[5]
    return (activation, activation_tan, adjoint, adjoint_tan, total_up.astype(jnp.bfloat16), total_down.astype(jnp.bfloat16))
```

```python
import functools

import jax
import jax.numpy as jnp
from jax import lax
from jax.experimental import pallas as pl
from jax.experimental.pallas import tpu as pltpu
from jax.sharding import PartitionSpec as P

sqrt_two_over_pi = 0.7978845608028654
cubic_coef = 0.044715
norm_eps = 1e-06


def gelu_parts(linear):
    inner_arg = sqrt_two_over_pi * (linear + cubic_coef * linear * linear * linear)
    first_slope = sqrt_two_over_pi * (1.0 + 3.0 * cubic_coef * linear * linear)
    second_slope = 6.0 * sqrt_two_over_pi * cubic_coef * linear
    tanh_value = jnp.tanh(inner_arg)
    sech_square = 1.0 - tanh_value * tanh_value
    gelu_value = 0.5 * linear * (1.0 + tanh_value)
    gelu_first = 0.5 * (1.0 + tanh_value) + 0.5 * linear * sech_square * first_slope
    gelu_second = sech_square * (
        first_slope - linear * tanh_value * first_slope * first_slope + 0.5 * linear * second_slope
    )
    return (gelu_value, gelu_first, gelu_second)


def matrix_product(left, right):
    return jnp.dot(left, right, preferred_element_type=jnp.float32)


def product_last(left, right):
    return lax.dot_general(
        left, right, (((1,), (1,)), ((), ())), preferred_element_type=jnp.float32
    )


def product_first(left, right):
    return lax.dot_general(
        left, right, (((0,), (0,)), ((), ())), preferred_element_type=jnp.float32
    )


f32, bf16 = (jnp.float32, jnp.bfloat16)
MESH = pl.DeviceIdType.MESH


def lane_chunk(size, wanted):
    fits = [c for c in range(128, wanted + 1, 128) if size % c == 0]
    return max(fits) if fits else size


def over_chunks(size, chunk, body):
    if size == chunk:
        body(pl.ds(0, size))
        return

    def step(index, carry):
        body(pl.ds(pl.multiple_of(index * chunk, chunk), chunk))
        return carry

    lax.fori_loop(0, size // chunk, step, 0)


def pair(value, tangent):
    blocks, rows, width = value.shape
    return jnp.stack([value, tangent], axis=1).reshape(blocks * 2 * rows, width)


def unpair(stacked, rows):
    wide = stacked.astype(f32).reshape(-1, 2, rows, stacked.shape[-1])
    return (wide[:, 0], wide[:, 1])


def norm_pair(stacked, gain, rows):
    values, values_tan = unpair(stacked, rows)
    inverse = lax.rsqrt(jnp.mean(values * values, axis=-1, keepdims=True) + norm_eps)
    inverse_tan = -(inverse * inverse * inverse) * jnp.mean(
        values * values_tan, axis=-1, keepdims=True
    )
    return (values * inverse * gain, (values_tan * inverse + values * inverse_tan) * gain)


def relay_kernel(
    sections, n_dp, ticks,
    carry_act, carry_act_tan, carry_adj, carry_adj_tan, fresh_act, loss_cot, stash_act,
    stash_act_tan, norm_gain, up_hbm, down_hbm, up_dir_hbm, down_dir_hbm,
    stash_out, adj_out, hidden_out, delta_out, final_out,
    up, down, up_dir, down_dir,
    left, left_dir, hid, hid_dir, slope, bend, hid_swap, delta, delta_dir, delta_swap,
    adj_dir, stash_all, gathered, outgoing, partial, from_core, to_chip, from_chip,
    weight_sems, out_sems, core_sems, chip_sems, shift_sems, relay_sems, stash_sems, stash_relay,
):
    chips = n_dp // 2
    rows = carry_act.shape[1]
    width = carry_act.shape[2]
    units = up.shape[1]
    band = n_dp * 2 * rows
    section, part = (lax.axis_index("section"), lax.axis_index("dp"))
    chip, core = (part // 2, part % 2)
    other = 1 - core
    after, before = (lax.rem(section + 1, sections), lax.rem(section + sections - 1, sections))
    partner = (section, chip * 2 + other)
    gain = norm_gain[...].astype(f32)

    def chip_at(step):
        return lax.rem(chip + step, chips)

    loads = [
        pltpu.make_async_copy(source.at[0], target, weight_sems.at[i])
        for i, (source, target) in enumerate(
            ((up_hbm, up), (up_dir_hbm, up_dir), (down_hbm, down), (down_dir_hbm, down_dir))
        )
    ]
    for load in loads:
        load.start()

    barrier = pltpu.get_barrier_semaphore()
    pl.semaphore_signal(barrier, inc=1, device_id=partner, device_id_type=MESH)
    for step in range(chips):
        place = chip_at(step) * 2 + core
        for where in (after, before):
            pl.semaphore_signal(barrier, inc=1, device_id=(where, place), device_id_type=MESH)
        if step:
            pl.semaphore_signal(barrier, inc=1, device_id=(section, place), device_id_type=MESH)

    def shift_copies(lane):
        where = after if lane % 2 == 0 else before
        return [
            pltpu.make_async_remote_copy(
                src_ref=outgoing.at[lane],
                dst_ref=gathered.at[lane, core, chip],
                send_sem=shift_sems.at[lane, 0, step],
                recv_sem=shift_sems.at[lane, 1, step],
                device_id=(where, chip_at(step) * 2 + core),
                device_id_type=MESH,
            )
            for step in range(chips)
        ]

    def relay_copy(lane):
        return pltpu.make_async_remote_copy(
            src_ref=gathered.at[lane, core],
            dst_ref=gathered.at[lane, core],
            send_sem=relay_sems.at[lane, 0],
            recv_sem=relay_sems.at[lane, 1],
            device_id=partner,
            device_id_type=MESH,
        )

    def stash_copies():
        return [
            pltpu.make_async_remote_copy(
                src_ref=stash_all.at[core, chip],
                dst_ref=stash_all.at[core, chip],
                send_sem=stash_sems.at[0, step],
                recv_sem=stash_sems.at[1, step],
                device_id=(section, chip_at(step) * 2 + core),
                device_id_type=MESH,
            )
            for step in range(1, chips)
        ]

    def stash_relay_copy():
        return pltpu.make_async_remote_copy(
            src_ref=stash_all.at[core],
            dst_ref=stash_all.at[core],
            send_sem=stash_relay.at[0],
            recv_sem=stash_relay.at[1],
            device_id=partner,
            device_id_type=MESH,
        )

    def core_copy(lane):
        return pltpu.make_async_remote_copy(
            src_ref=partial.at[lane, other],
            dst_ref=from_core.at[lane],
            send_sem=core_sems.at[lane, 0],
            recv_sem=core_sems.at[lane, 1],
            device_id=partner,
            device_id_type=MESH,
        )

    def chip_copies(lane):
        return [
            pltpu.make_async_remote_copy(
                src_ref=to_chip.at[lane, step - 1],
                dst_ref=from_chip.at[lane, step - 1],
                send_sem=chip_sems.at[lane, 0, step - 1],
                recv_sem=chip_sems.at[lane, 1, step - 1],
                device_id=(section, chip_at(step) * 2 + core),
                device_id_type=MESH,
            )
            for step in range(1, chips)
        ]

    def start_all(copies):
        for copy in copies:
            copy.start()

    def stage_shift(lane, value, tangent):
        tick = lane // 2
        if lane % 2 == 0:
            ends, entering = (section == sections - 1, fresh_act[tick])
        else:
            ends, entering = (section == 0, loss_cot[tick])
        value = jnp.where(ends, entering.astype(f32), value)
        tangent = jnp.where(ends, 0.0, tangent)
        outgoing[lane] = pair(value[None], tangent[None]).astype(bf16)

    def relay(lane):
        for copy in shift_copies(lane):
            copy.wait_recv()
        relay_copy(lane).start()

    def reduce_in_chip(lane):
        core_copy(lane).wait_recv()
        for step in range(1, chips):
            place = chip_at(step)
            summed = partial[lane, core, place].astype(f32) + from_core[lane, place].astype(f32)
            to_chip[lane, step - 1] = summed.astype(bf16)
        start_all(chip_copies(lane))

    def reduced(lane):
        total = partial[lane, core, chip].astype(f32) + from_core[lane, chip].astype(f32)
        for step, copy in enumerate(chip_copies(lane)):
            copy.wait_recv()
            total = total + from_chip[lane, step].astype(f32)
        return (total[:rows], total[rows:])

    stage_shift(0, carry_act[0].astype(f32), carry_act_tan[0].astype(f32))
    pl.semaphore_wait(barrier, 3 * chips)
    start_all(shift_copies(0))
    stage_shift(1, carry_adj[0].astype(f32), carry_adj_tan[0].astype(f32))
    start_all(shift_copies(1))
    for tick in range(ticks):
        stacked = pair(
            stash_act[0, tick].astype(f32)[None], stash_act_tan[0, tick].astype(f32)[None]
        )
        normed, normed_tan = norm_pair(stacked, gain, rows)
        stash_all[core, chip, tick] = pair(normed, normed_tan).astype(bf16)
    start_all(stash_copies())
    relay(0)
    relay(1)
    for copy in stash_copies():
        copy.wait_recv()
    stash_relay_copy().start()

    outs = []

    def send_out(source, target):
        copy = pltpu.make_async_copy(source, target, out_sems.at[len(outs)])
        copy.start()
        outs.append(copy)

    def stage_forward(tick):
        lane = 2 * tick
        relay_copy(lane).wait_recv()
        for block in range(n_dp):
            where = pl.ds(block * 2 * rows, 2 * rows)
            normed, normed_tan = norm_pair(
                gathered[lane, block // chips, block % chips], gain, rows
            )
            left[where, :] = pair(normed, normed_tan).astype(bf16)
            left_dir[where, :] = pair(jnp.zeros_like(normed), normed).astype(bf16)

    stage_forward(0)
    stash_relay_copy().wait_recv()
    for block in range(n_dp):
        for tick in range(ticks):
            where = pl.ds(band + (block * ticks + tick) * 2 * rows, 2 * rows)
            stacked = stash_all[block // chips, block % chips, tick]
            left[where, :] = stacked
            value = unpair(stacked, rows)[0]
            left_dir[where, :] = pair(jnp.zeros_like(value), value).astype(bf16)
    send_out(stash_all, stash_out)
    loads[0].wait()
    loads[1].wait()

    unit_chunk = lane_chunk(units, 384)
    width_chunk = lane_chunk(width, 768)

    def up_products(height, with_stash, cols):
        stacked = matrix_product(left[:height, :], up[:, cols]) + matrix_product(
            left_dir[:height, :], up_dir[:, cols]
        )
        linear, linear_tan = unpair(stacked[:band], rows)
        value, first, _ = gelu_parts(linear)
        hid[:, cols] = pair(value, first * linear_tan).astype(bf16)
        hid_dir[:, cols] = pair(jnp.zeros_like(value), value).astype(bf16)
        if with_stash:
            linear, linear_tan = unpair(stacked[band:], rows)
            value, first, second = gelu_parts(linear)
            hid_swap[:, cols] = pair(first * linear_tan, value).astype(bf16)
            by_tick = (n_dp, ticks, rows, value.shape[-1])
            slope[:, :, :, cols] = first.reshape(by_tick)
            bend[:, :, :, cols] = (second * linear_tan).reshape(by_tick)

    def down_products(lane, cols):
        stacked = matrix_product(hid[...], down[:, cols]) + matrix_product(
            hid_dir[...], down_dir[:, cols]
        )
        partial[lane, :, :, :, cols] = stacked.astype(bf16).reshape(2, chips, 2 * rows, -1)

    def adjoint_products(tick, cols):
        adjoint = gathered[2 * tick + 1].reshape(band, width)
        stacked = product_last(adjoint, down[cols, :]) + product_last(
            adj_dir[...], down_dir[cols, :]
        )
        upstream, upstream_tan = unpair(stacked, rows)
        first, second_tan = (slope[:, tick, :, cols], bend[:, tick, :, cols])
        value = upstream * first
        tangent = upstream_tan * first + upstream * second_tan
        delta[:, cols] = pair(value, tangent).astype(bf16)
        delta_dir[:, cols] = pair(jnp.zeros_like(value), value).astype(bf16)
        delta_swap[:, tick, :, cols] = (
            pair(tangent, value).astype(bf16).reshape(n_dp, 2 * rows, -1)
        )

    def back_products(lane, cols):
        stacked = product_last(delta[...], up[cols, :]) + product_last(
            delta_dir[...], up_dir[cols, :]
        )
        partial[lane, :, :, :, cols] = stacked.astype(bf16).reshape(2, chips, 2 * rows, -1)

    def finish_forward(tick):
        lane = 2 * tick
        value, tangent = reduced(lane)
        own = gathered[lane, core, chip].astype(f32)
        value, tangent = (own[:rows] + value, own[rows:] + tangent)
        if tick + 1 < ticks:
            stage_shift(lane + 2, value, tangent)
            start_all(shift_copies(lane + 2))
        else:
            final_out[0] = value.astype(bf16)
            final_out[1] = tangent.astype(bf16)

    def finish_backward(tick):
        lane = 2 * tick + 1
        summed, summed_tan = reduced(lane)
        arriving = gathered[lane, core, chip].astype(f32)
        values = stash_act[0, tick].astype(f32)
        values_tan = stash_act_tan[0, tick].astype(f32)
        inverse = lax.rsqrt(jnp.mean(values * values, axis=-1, keepdims=True) + norm_eps)
        cube = inverse * inverse * inverse
        inverse_tan = -cube * jnp.mean(values * values_tan, axis=-1, keepdims=True)
        weighted, weighted_tan = (summed * gain, summed_tan * gain)
        moment = jnp.mean(values * weighted, axis=-1, keepdims=True)
        moment_tan = jnp.mean(
            values_tan * weighted + values * weighted_tan, axis=-1, keepdims=True
        )
        value = arriving[:rows] + inverse * weighted - cube * values * moment
        tangent = (
            arriving[rows:]
            + inverse_tan * weighted
            + inverse * weighted_tan
            - 3.0 * inverse * inverse * inverse_tan * values * moment
            - cube * values_tan * moment
            - cube * values * moment_tan
        )
        if tick + 1 < ticks:
            stage_shift(lane + 2, value, tangent)
            start_all(shift_copies(lane + 2))
        else:
            final_out[2] = value.astype(bf16)
            final_out[3] = tangent.astype(bf16)

    for tick in range(ticks):
        ahead, behind = (2 * tick, 2 * tick + 1)
        if tick:
            stage_forward(tick)
        height = left.shape[0] if tick == 0 else band
        over_chunks(units, unit_chunk, functools.partial(up_products, height, tick == 0))
        if tick == 0:
            send_out(hid_swap, hidden_out)
            loads[2].wait()
            loads[3].wait()
        else:
            relay(behind)
        over_chunks(width, width_chunk, functools.partial(down_products, ahead))
        core_copy(ahead).start()
        relay_copy(behind).wait_recv()
        for block in range(n_dp):
            value = unpair(gathered[behind, block // chips, block % chips], rows)[0]
            adj_dir[pl.ds(block * 2 * rows, 2 * rows), :] = pair(
                jnp.zeros_like(value), value
            ).astype(bf16)
        send_out(gathered.at[behind], adj_out.at[tick])
        over_chunks(units, unit_chunk, functools.partial(adjoint_products, tick))
        reduce_in_chip(ahead)
        over_chunks(width, width_chunk, functools.partial(back_products, behind))
        core_copy(behind).start()
        finish_forward(tick)
        reduce_in_chip(behind)
        if tick + 1 < ticks:
            relay(ahead + 2)
        else:
            send_out(delta_swap, delta_out)
        finish_backward(tick)

    for lane in range(2 * ticks):
        for copy in shift_copies(lane) + chip_copies(lane):
            copy.wait_send()
        relay_copy(lane).wait_send()
        core_copy(lane).wait_send()
    for copy in stash_copies():
        copy.wait_send()
    stash_relay_copy().wait_send()
    for copy in outs:
        copy.wait()


def curvature_kernel(split_units, stash_sw, delta_sw, hidden_sw, adj, final, *outs):
    act, act_tan, adj_new, adj_new_tan, up_out, down_out = outs
    for index, target in enumerate((act, act_tan, adj_new, adj_new_tan)):
        target[0] = final[index]
    up_out[0] = product_first(stash_sw[...], delta_sw[...]).astype(bf16)

    def down():
        down_out[0] = product_first(hidden_sw[...], adj[...]).astype(bf16)

    if split_units:
        down()
    else:
        pl.when(pl.program_id(0) == 0)(down)


def shards(
    carry_act, carry_act_tan, carry_adj, carry_adj_tan, fresh_act, loss_cot, stash_act,
    stash_act_tan, norm_gain, up_weight, down_weight, up_dir, down_dir,
):
    sections, n_dp = (lax.axis_size("section"), lax.axis_size("dp"))
    chips = n_dp // 2
    ticks, rows, width = fresh_act.shape
    units = up_weight.shape[2]
    band = n_dp * 2 * rows
    tall = band * (1 + ticks)
    lanes = 2 * ticks
    vmem, anywhere = (
        pl.BlockSpec(memory_space=pltpu.VMEM),
        pl.BlockSpec(memory_space=pl.ANY),
    )
    block = (2 * rows, width)
    stash_out, adj_out, hidden_out, delta_out, final_out = pl.pallas_call(
        functools.partial(relay_kernel, sections, n_dp, ticks),
        out_shape=(
            jax.ShapeDtypeStruct((2, chips, ticks) + block, bf16),
            jax.ShapeDtypeStruct((ticks, 2, chips) + block, bf16),
            jax.ShapeDtypeStruct((band * ticks, units), bf16),
            jax.ShapeDtypeStruct((n_dp, ticks, 2 * rows, units), bf16),
            jax.ShapeDtypeStruct((4, rows, width), bf16),
        ),
        in_specs=[vmem] * 9 + [anywhere] * 4,
        out_specs=(anywhere,) * 4 + (vmem,),
        scratch_shapes=[
            pltpu.VMEM((width, units), bf16),
            pltpu.VMEM((units, width), bf16),
            pltpu.VMEM((width, units), bf16),
            pltpu.VMEM((units, width), bf16),
            pltpu.VMEM((tall, width), bf16),
            pltpu.VMEM((tall, width), bf16),
            pltpu.VMEM((band, units), bf16),
            pltpu.VMEM((band, units), bf16),
            pltpu.VMEM((n_dp, ticks, rows, units), f32),
            pltpu.VMEM((n_dp, ticks, rows, units), f32),
            pltpu.VMEM((band * ticks, units), bf16),
            pltpu.VMEM((band, units), bf16),
            pltpu.VMEM((band, units), bf16),
            pltpu.VMEM((n_dp, ticks, 2 * rows, units), bf16),
            pltpu.VMEM((band, width), bf16),
            pltpu.VMEM((2, chips, ticks) + block, bf16),
            pltpu.VMEM((lanes, 2, chips) + block, bf16),
            pltpu.VMEM((lanes,) + block, bf16),
            pltpu.VMEM((lanes, 2, chips) + block, bf16),
            pltpu.VMEM((lanes, chips) + block, bf16),
            pltpu.VMEM((lanes, chips - 1) + block, bf16),
            pltpu.VMEM((lanes, chips - 1) + block, bf16),
            pltpu.SemaphoreType.DMA((4,)),
            pltpu.SemaphoreType.DMA((3 + ticks,)),
            pltpu.SemaphoreType.DMA((lanes, 2)),
            pltpu.SemaphoreType.DMA((lanes, 2, chips - 1)),
            pltpu.SemaphoreType.DMA((lanes, 2, chips)),
            pltpu.SemaphoreType.DMA((lanes, 2)),
            pltpu.SemaphoreType.DMA((2, chips)),
            pltpu.SemaphoreType.DMA((2,)),
        ],
        compiler_params=pltpu.CompilerParams(
            collective_id=0, has_side_effects=True, vmem_limit_bytes=60 * 1024 * 1024
        ),
        name="relay",
    )(
        carry_act, carry_act_tan, carry_adj, carry_adj_tan, fresh_act, loss_cot, stash_act,
        stash_act_tan, norm_gain, up_weight, down_weight, up_dir, down_dir,
    )
    deep = band * ticks
    stash_sw = stash_out.reshape(deep, width)
    delta_sw = delta_out.reshape(deep, units)
    adj_flat = jnp.swapaxes(adj_out.reshape(ticks, n_dp, 2 * rows, width), 0, 1).reshape(deep, width)
    width_chunk = lane_chunk(width, 256)
    steps = width // width_chunk
    split_units = units % (128 * steps) == 0
    unit_chunk = units // steps if split_units else units
    unit_index = (lambda i: i) if split_units else (lambda i: 0)
    whole = lambda *shape: pl.BlockSpec(shape, lambda i: (0,) * len(shape))
    rows_shape = jax.ShapeDtypeStruct((1, rows, width), bf16)
    return tuple(
        pl.pallas_call(
            functools.partial(curvature_kernel, split_units),
            grid=(steps,),
            out_shape=(rows_shape,) * 4
            + (
                jax.ShapeDtypeStruct((1, width, units), bf16),
                jax.ShapeDtypeStruct((1, units, width), bf16),
            ),
            in_specs=[
                pl.BlockSpec((deep, width_chunk), lambda i: (0, i)),
                whole(deep, units),
                pl.BlockSpec((deep, unit_chunk), lambda i: (0, unit_index(i))),
                whole(deep, width),
                whole(4, rows, width),
            ],
            out_specs=(whole(1, rows, width),) * 4
            + (
                pl.BlockSpec((1, width_chunk, units), lambda i: (0, i, 0)),
                pl.BlockSpec((1, unit_chunk, width), lambda i: (0, unit_index(i), 0)),
            ),
            name="curvature",
        )(stash_sw, delta_sw, hidden_out, adj_flat, final_out)
    )


def solution(mesh):
    in_specs = (
        P("section", "dp", None),
        P("section", "dp", None),
        P("section", "dp", None),
        P("section", "dp", None),
        P(None, "dp", None),
        P(None, "dp", None),
        P("section", None, "dp", None),
        P("section", None, "dp", None),
        P("section", None),
        P("section", None, "dp"),
        P("section", "dp", None),
        P("section", None, "dp"),
        P("section", "dp", None),
    )
    out_specs = (
        P("section", "dp", None),
        P("section", "dp", None),
        P("section", "dp", None),
        P("section", "dp", None),
        P("section", None, "dp"),
        P("section", "dp", None),
    )
    return jax.shard_map(shards, mesh=mesh, in_specs=in_specs, out_specs=out_specs, check_vma=False)
```

```python
import functools

import jax
import jax.numpy as jnp
from jax import lax
from jax.experimental import pallas as pl
from jax.experimental.pallas import tpu as pltpu
from jax.sharding import PartitionSpec as P

sqrt_two_over_pi = 0.7978845608028654
cubic_coef = 0.044715
norm_eps = 1e-06


def gelu_parts(linear):
    inner_arg = sqrt_two_over_pi * (linear + cubic_coef * linear * linear * linear)
    first_slope = sqrt_two_over_pi * (1.0 + 3.0 * cubic_coef * linear * linear)
    second_slope = 6.0 * sqrt_two_over_pi * cubic_coef * linear
    tanh_value = jnp.tanh(inner_arg)
    sech_square = 1.0 - tanh_value * tanh_value
    gelu_value = 0.5 * linear * (1.0 + tanh_value)
    gelu_first = 0.5 * (1.0 + tanh_value) + 0.5 * linear * sech_square * first_slope
    gelu_second = sech_square * (
        first_slope - linear * tanh_value * first_slope * first_slope + 0.5 * linear * second_slope
    )
    return (gelu_value, gelu_first, gelu_second)


def matrix_product(left, right):
    return jnp.dot(left, right, preferred_element_type=jnp.float32)


def product_last(left, right):
    return lax.dot_general(
        left, right, (((1,), (1,)), ((), ())), preferred_element_type=jnp.float32
    )


def product_first(left, right):
    return lax.dot_general(
        left, right, (((0,), (0,)), ((), ())), preferred_element_type=jnp.float32
    )


f32, bf16 = (jnp.float32, jnp.bfloat16)
MESH = pl.DeviceIdType.MESH


def lane_chunk(size, wanted):
    fits = [c for c in range(128, wanted + 1, 128) if size % c == 0]
    return max(fits) if fits else size


def over_chunks(size, chunk, body, after=None):
    count = size // chunk

    def step(index, carry):
        start = index * chunk if count == 1 else pl.multiple_of(index * chunk, chunk)
        body(pl.ds(start, chunk))
        if after is not None:
            after(index)
        return carry

    if count == 1:
        step(0, 0)
    else:
        lax.fori_loop(0, count, step, 0)


def once(index, wanted, work):
    if isinstance(index, int):
        if index == wanted:
            work()
    else:
        pl.when(index == wanted)(work)


def pair(value, tangent):
    blocks, rows, width = value.shape
    return jnp.stack([value, tangent], axis=1).reshape(blocks * 2 * rows, width)


def unpair(stacked, rows):
    wide = stacked.astype(f32).reshape(-1, 2, rows, stacked.shape[-1])
    return (wide[:, 0], wide[:, 1])


def norm_pair(stacked, gain, rows):
    values, values_tan = unpair(stacked, rows)
    inverse = lax.rsqrt(jnp.mean(values * values, axis=-1, keepdims=True) + norm_eps)
    inverse_tan = -(inverse * inverse * inverse) * jnp.mean(
        values * values_tan, axis=-1, keepdims=True
    )
    return (values * inverse * gain, (values_tan * inverse + values * inverse_tan) * gain)


def relay_kernel(
    sections, n_dp, ticks,
    carry_act, carry_act_tan, carry_adj, carry_adj_tan, fresh_act, loss_cot, stash_act,
    stash_act_tan, norm_gain, up_hbm, down_hbm, up_dir_hbm, down_dir_hbm,
    stash_out, adj_out, hidden_out, delta_out, final_out,
    up, down, up_dir, down_dir,
    left, left_dir, hid, hid_dir, slope, bend, hid_swap, delta, delta_dir, delta_swap,
    adj_dir, stash_all, gathered, outgoing, partial, from_core, to_chip, from_chip,
    weight_sems, out_sems, core_sems, chip_sems, shift_sems, relay_sems, stash_sems, stash_relay,
):
    chips = n_dp // 2
    rows = carry_act.shape[1]
    width = carry_act.shape[2]
    units = up.shape[1]
    band = n_dp * 2 * rows
    unit_chunk = lane_chunk(units, 384)
    width_chunk = lane_chunk(width, 768)
    pieces = width // width_chunk
    section, part = (lax.axis_index("section"), lax.axis_index("dp"))
    chip, core = (part // 2, part % 2)
    other = 1 - core
    after, before = (lax.rem(section + 1, sections), lax.rem(section + sections - 1, sections))
    partner = (section, chip * 2 + other)
    gain = norm_gain[...].astype(f32)

    def chip_at(step):
        return lax.rem(chip + step, chips)

    loads = [
        pltpu.make_async_copy(source.at[0], target, weight_sems.at[i])
        for i, (source, target) in enumerate(
            ((up_hbm, up), (up_dir_hbm, up_dir), (down_hbm, down), (down_dir_hbm, down_dir))
        )
    ]
    for load in loads:
        load.start()

    barrier = pltpu.get_barrier_semaphore()
    pl.semaphore_signal(barrier, inc=1, device_id=partner, device_id_type=MESH)
    for step in range(chips):
        place = chip_at(step) * 2 + core
        for where in (after, before):
            pl.semaphore_signal(barrier, inc=1, device_id=(where, place), device_id_type=MESH)
        if step:
            pl.semaphore_signal(barrier, inc=1, device_id=(section, place), device_id_type=MESH)

    def shift_copies(lane):
        where = after if lane % 2 == 0 else before
        return [
            pltpu.make_async_remote_copy(
                src_ref=outgoing.at[lane],
                dst_ref=gathered.at[lane, core, chip],
                send_sem=shift_sems.at[lane, 0, step],
                recv_sem=shift_sems.at[lane, 1, step],
                device_id=(where, chip_at(step) * 2 + core),
                device_id_type=MESH,
            )
            for step in range(chips)
        ]

    def relay_copy(lane):
        return pltpu.make_async_remote_copy(
            src_ref=gathered.at[lane, core],
            dst_ref=gathered.at[lane, core],
            send_sem=relay_sems.at[lane, 0],
            recv_sem=relay_sems.at[lane, 1],
            device_id=partner,
            device_id_type=MESH,
        )

    def stash_copies(tick):
        return [
            pltpu.make_async_remote_copy(
                src_ref=stash_all.at[tick, core, chip],
                dst_ref=stash_all.at[tick, core, chip],
                send_sem=stash_sems.at[tick, 0, step],
                recv_sem=stash_sems.at[tick, 1, step],
                device_id=(section, chip_at(step) * 2 + core),
                device_id_type=MESH,
            )
            for step in range(1, chips)
        ]

    def stash_relay_copy(tick):
        return pltpu.make_async_remote_copy(
            src_ref=stash_all.at[tick, core],
            dst_ref=stash_all.at[tick, core],
            send_sem=stash_relay.at[tick, 0],
            recv_sem=stash_relay.at[tick, 1],
            device_id=partner,
            device_id_type=MESH,
        )

    def relay_stash(tick):
        for copy in stash_copies(tick):
            copy.wait_recv()
        stash_relay_copy(tick).start()

    def columns(piece):
        if isinstance(piece, int):
            return pl.ds(piece * width_chunk, width_chunk)
        return pl.ds(pl.multiple_of(piece * width_chunk, width_chunk), width_chunk)

    def core_copy(lane, piece):
        return pltpu.make_async_remote_copy(
            src_ref=partial.at[lane, other, :, :, columns(piece)],
            dst_ref=from_core.at[lane, :, :, columns(piece)],
            send_sem=core_sems.at[lane, piece, 0],
            recv_sem=core_sems.at[lane, piece, 1],
            device_id=partner,
            device_id_type=MESH,
        )

    def chip_copies(lane, piece):
        return [
            pltpu.make_async_remote_copy(
                src_ref=to_chip.at[lane, step - 1, :, columns(piece)],
                dst_ref=from_chip.at[lane, step - 1, :, columns(piece)],
                send_sem=chip_sems.at[lane, piece, 0, step - 1],
                recv_sem=chip_sems.at[lane, piece, 1, step - 1],
                device_id=(section, chip_at(step) * 2 + core),
                device_id_type=MESH,
            )
            for step in range(1, chips)
        ]

    def start_all(copies):
        for copy in copies:
            copy.start()

    def stage_shift(lane, value, tangent):
        tick = lane // 2
        if lane % 2 == 0:
            ends, entering = (section == sections - 1, fresh_act[tick])
        else:
            ends, entering = (section == 0, loss_cot[tick])
        value = jnp.where(ends, entering.astype(f32), value)
        tangent = jnp.where(ends, 0.0, tangent)
        outgoing[lane] = pair(value[None], tangent[None]).astype(bf16)

    def relay(lane):
        for copy in shift_copies(lane):
            copy.wait_recv()
        relay_copy(lane).start()

    def reduce_in_chip(lane, piece):
        core_copy(lane, piece).wait_recv()
        cols = columns(piece)
        for step in range(1, chips):
            place = chip_at(step)
            summed = partial[lane, core, place, :, cols].astype(f32)
            summed = summed + from_core[lane, place, :, cols].astype(f32)
            to_chip[lane, step - 1, :, cols] = summed.astype(bf16)
        start_all(chip_copies(lane, piece))

    def reduced(lane):
        for piece in range(pieces):
            for copy in chip_copies(lane, piece):
                copy.wait_recv()
        total = partial[lane, core, chip].astype(f32) + from_core[lane, chip].astype(f32)
        for step in range(chips - 1):
            total = total + from_chip[lane, step].astype(f32)
        return (total[:rows], total[rows:])

    def norm_stash(tick):
        stacked = pair(
            stash_act[0, tick].astype(f32)[None], stash_act_tan[0, tick].astype(f32)[None]
        )
        normed, normed_tan = norm_pair(stacked, gain, rows)
        stash_all[tick, core, chip] = pair(normed, normed_tan).astype(bf16)

    stage_shift(0, carry_act[0].astype(f32), carry_act_tan[0].astype(f32))
    norm_stash(0)
    pl.semaphore_wait(barrier, 3 * chips)
    start_all(shift_copies(0))
    start_all(stash_copies(0))
    stage_shift(1, carry_adj[0].astype(f32), carry_adj_tan[0].astype(f32))
    for tick in range(1, ticks):
        norm_stash(tick)
    relay_stash(0)
    relay(0)
    start_all(shift_copies(1))
    for tick in range(1, ticks):
        start_all(stash_copies(tick))

    outs = []

    def send_out(source, target):
        copy = pltpu.make_async_copy(source, target, out_sems.at[len(outs)])
        copy.start()
        outs.append(copy)

    def stage_forward(tick):
        lane = 2 * tick
        relay_copy(lane).wait_recv()
        for block in range(n_dp):
            where = pl.ds(block * 2 * rows, 2 * rows)
            normed, normed_tan = norm_pair(
                gathered[lane, block // chips, block % chips], gain, rows
            )
            left[where, :] = pair(normed, normed_tan).astype(bf16)
            left_dir[where, :] = pair(jnp.zeros_like(normed), normed).astype(bf16)

    def stage_stash(tick):
        stash_relay_copy(tick).wait_recv()
        for block in range(n_dp):
            where = pl.ds(band + block * 2 * rows, 2 * rows)
            stacked = stash_all[tick, block // chips, block % chips]
            left[where, :] = stacked
            value = unpair(stacked, rows)[0]
            left_dir[where, :] = pair(jnp.zeros_like(value), value).astype(bf16)
        send_out(stash_all.at[tick], stash_out.at[tick])

    def up_products(forward, stash_tick, cols):
        low = 0 if forward else band
        high = band if stash_tick is None else 2 * band
        stacked = matrix_product(left[low:high, :], up[:, cols]) + matrix_product(
            left_dir[low:high, :], up_dir[:, cols]
        )
        if forward:
            linear, linear_tan = unpair(stacked[:band], rows)
            value, first, _ = gelu_parts(linear)
            hid[:, cols] = pair(value, first * linear_tan).astype(bf16)
            hid_dir[:, cols] = pair(jnp.zeros_like(value), value).astype(bf16)
        if stash_tick is not None:
            linear, linear_tan = unpair(stacked[band - low :], rows)
            value, first, second = gelu_parts(linear)
            hid_swap[stash_tick, :, cols] = pair(first * linear_tan, value).astype(bf16)
            slope[stash_tick, :, :, cols] = first
            bend[stash_tick, :, :, cols] = second * linear_tan

    def down_products(lane, cols):
        stacked = matrix_product(hid[...], down[:, cols]) + matrix_product(
            hid_dir[...], down_dir[:, cols]
        )
        partial[lane, :, :, :, cols] = stacked.astype(bf16).reshape(2, chips, 2 * rows, -1)

    def adjoint_products(tick, cols):
        adjoint = gathered[2 * tick + 1].reshape(band, width)
        stacked = product_last(adjoint, down[cols, :]) + product_last(
            adj_dir[...], down_dir[cols, :]
        )
        upstream, upstream_tan = unpair(stacked, rows)
        first, second_tan = (slope[tick, :, :, cols], bend[tick, :, :, cols])
        value = upstream * first
        tangent = upstream_tan * first + upstream * second_tan
        delta[:, cols] = pair(value, tangent).astype(bf16)
        delta_dir[:, cols] = pair(jnp.zeros_like(value), value).astype(bf16)
        delta_swap[tick, :, cols] = pair(tangent, value).astype(bf16)

    def back_products(lane, cols):
        stacked = product_last(delta[...], up[cols, :]) + product_last(
            delta_dir[...], up_dir[cols, :]
        )
        partial[lane, :, :, :, cols] = stacked.astype(bf16).reshape(2, chips, 2 * rows, -1)

    def finish_forward(tick):
        lane = 2 * tick
        value, tangent = reduced(lane)
        own = gathered[lane, core, chip].astype(f32)
        value, tangent = (own[:rows] + value, own[rows:] + tangent)
        if tick + 1 < ticks:
            stage_shift(lane + 2, value, tangent)
            start_all(shift_copies(lane + 2))
        else:
            final_out[0] = value.astype(bf16)
            final_out[1] = tangent.astype(bf16)

    def finish_backward(tick):
        lane = 2 * tick + 1
        summed, summed_tan = reduced(lane)
        arriving = gathered[lane, core, chip].astype(f32)
        values = stash_act[0, tick].astype(f32)
        values_tan = stash_act_tan[0, tick].astype(f32)
        inverse = lax.rsqrt(jnp.mean(values * values, axis=-1, keepdims=True) + norm_eps)
        cube = inverse * inverse * inverse
        inverse_tan = -cube * jnp.mean(values * values_tan, axis=-1, keepdims=True)
        weighted, weighted_tan = (summed * gain, summed_tan * gain)
        moment = jnp.mean(values * weighted, axis=-1, keepdims=True)
        moment_tan = jnp.mean(
            values_tan * weighted + values * weighted_tan, axis=-1, keepdims=True
        )
        value = arriving[:rows] + inverse * weighted - cube * values * moment
        tangent = (
            arriving[rows:]
            + inverse_tan * weighted
            + inverse * weighted_tan
            - 3.0 * inverse * inverse * inverse_tan * values * moment
            - cube * values_tan * moment
            - cube * values * moment_tan
        )
        if tick + 1 < ticks:
            stage_shift(lane + 2, value, tangent)
            start_all(shift_copies(lane + 2))
        else:
            final_out[2] = value.astype(bf16)
            final_out[3] = tangent.astype(bf16)

    def call(work, *given):
        return functools.partial(work, *given)

    def start_piece(lane, piece):
        core_copy(lane, piece).start()

    def stage_adjoint(tick):
        lane = 2 * tick + 1
        relay_copy(lane).wait_recv()
        for block in range(n_dp):
            value = unpair(gathered[lane, block // chips, block % chips], rows)[0]
            adj_dir[pl.ds(block * 2 * rows, 2 * rows), :] = pair(
                jnp.zeros_like(value), value
            ).astype(bf16)
        send_out(gathered.at[lane], adj_out.at[tick])

    stage_forward(0)
    stage_stash(0)
    loads[0].wait()
    loads[1].wait()
    last = pieces - 1
    for tick in range(ticks):
        ahead, behind = (2 * tick, 2 * tick + 1)
        if tick:
            stage_forward(tick)
        over_chunks(units, unit_chunk, call(up_products, True, None if tick else 0))
        if tick == 0:
            send_out(hid_swap.at[0], hidden_out.at[0])
            loads[2].wait()
            loads[3].wait()
        over_chunks(width, width_chunk, call(down_products, ahead), call(start_piece, ahead))
        relay(behind)
        stage_adjoint(tick)

        def reduce_pieces(index):
            def all_pieces():
                for piece in range(pieces):
                    reduce_in_chip(ahead, piece)

            once(index, 0, all_pieces)

        over_chunks(units, unit_chunk, call(adjoint_products, tick), reduce_pieces)
        send_out(delta_swap.at[tick], delta_out.at[tick])
        finish_forward(tick)
        if tick + 1 < ticks:
            relay_stash(tick + 1)

        def pass_piece(index):
            start_piece(behind, index)
            for piece in range(1, pieces):
                once(index, piece, call(reduce_in_chip, behind, piece - 1))

        over_chunks(width, width_chunk, call(back_products, behind), pass_piece)
        if tick + 1 < ticks:
            reduce_in_chip(behind, last)
            stage_stash(tick + 1)
            over_chunks(units, unit_chunk, call(up_products, False, tick + 1))
            send_out(hid_swap.at[tick + 1], hidden_out.at[tick + 1])
            relay(ahead + 2)
        else:
            reduce_in_chip(behind, last)
        finish_backward(tick)

    for lane in range(2 * ticks):
        for copy in shift_copies(lane):
            copy.wait_send()
        relay_copy(lane).wait_send()
        for piece in range(pieces):
            core_copy(lane, piece).wait_send()
            for copy in chip_copies(lane, piece):
                copy.wait_send()
    for tick in range(ticks):
        for copy in stash_copies(tick):
            copy.wait_send()
        stash_relay_copy(tick).wait_send()
    for copy in outs:
        copy.wait()


def curvature_kernel(
    stash_hbm, delta_hbm, hidden_hbm, adj_hbm, final_hbm,
    act, act_tan, adj_new, adj_new_tan, up_hbm, down_hbm,
    stash_sw, delta_sw, hidden_sw, adj, final, up_out, down_out, in_sems, row_sems, up_sems, down_sems,
):
    sources = (stash_hbm, delta_hbm, hidden_hbm, adj_hbm, final_hbm)
    targets = (stash_sw, delta_sw, hidden_sw, adj, final)
    loads = [
        pltpu.make_async_copy(source, target, in_sems.at[i])
        for i, (source, target) in enumerate(zip(sources, targets))
    ]
    for load in loads:
        load.start()
    for load in loads:
        load.wait()
    row_copies = [
        pltpu.make_async_copy(final.at[i], target.at[0], row_sems.at[i])
        for i, target in enumerate((act, act_tan, adj_new, adj_new_tan))
    ]
    for copy in row_copies:
        copy.start()

    def product(left, right, out, target, sems):
        chunk = out.shape[0] // sems.shape[0]

        def part(piece):
            where = pl.ds(piece * chunk, chunk)
            if not isinstance(piece, int):
                where = pl.ds(pl.multiple_of(piece * chunk, chunk), chunk)
            out[where, :] = product_first(left[:, where], right[...]).astype(bf16)
            copy = pltpu.make_async_copy(out.at[where, :], target.at[0, where, :], sems.at[piece])
            copy.start()

        return part

    up_part = product(stash_sw, delta_sw, up_out, up_hbm, up_sems)
    down_part = product(hidden_sw, adj, down_out, down_hbm, down_sems)
    if up_sems.shape[0] == down_sems.shape[0] > 1:

        def step(piece, carry):
            up_part(piece)
            down_part(piece)
            return carry

        lax.fori_loop(0, up_sems.shape[0], step, 0)
    else:
        for piece in range(up_sems.shape[0]):
            up_part(piece)
        for piece in range(down_sems.shape[0]):
            down_part(piece)
    for out, target, sems in ((up_out, up_hbm, up_sems), (down_out, down_hbm, down_sems)):
        chunk = out.shape[0] // sems.shape[0]
        for piece in range(sems.shape[0]):
            where = pl.ds(piece * chunk, chunk)
            pltpu.make_async_copy(out.at[where, :], target.at[0, where, :], sems.at[piece]).wait()
    for copy in row_copies:
        copy.wait()


def shards(
    carry_act, carry_act_tan, carry_adj, carry_adj_tan, fresh_act, loss_cot, stash_act,
    stash_act_tan, norm_gain, up_weight, down_weight, up_dir, down_dir,
):
    sections, n_dp = (lax.axis_size("section"), lax.axis_size("dp"))
    chips = n_dp // 2
    ticks, rows, width = fresh_act.shape
    units = up_weight.shape[2]
    band = n_dp * 2 * rows
    tall = 2 * band
    pieces = width // lane_chunk(width, 768)
    lanes = 2 * ticks
    vmem, anywhere = (
        pl.BlockSpec(memory_space=pltpu.VMEM),
        pl.BlockSpec(memory_space=pl.ANY),
    )
    block = (2 * rows, width)
    stash_out, adj_out, hidden_out, delta_out, final_out = pl.pallas_call(
        functools.partial(relay_kernel, sections, n_dp, ticks),
        out_shape=(
            jax.ShapeDtypeStruct((ticks, 2, chips) + block, bf16),
            jax.ShapeDtypeStruct((ticks, 2, chips) + block, bf16),
            jax.ShapeDtypeStruct((ticks, band, units), bf16),
            jax.ShapeDtypeStruct((ticks, band, units), bf16),
            jax.ShapeDtypeStruct((4, rows, width), bf16),
        ),
        in_specs=[vmem] * 9 + [anywhere] * 4,
        out_specs=(anywhere,) * 4 + (vmem,),
        scratch_shapes=[
            pltpu.VMEM((width, units), bf16),
            pltpu.VMEM((units, width), bf16),
            pltpu.VMEM((width, units), bf16),
            pltpu.VMEM((units, width), bf16),
            pltpu.VMEM((tall, width), bf16),
            pltpu.VMEM((tall, width), bf16),
            pltpu.VMEM((band, units), bf16),
            pltpu.VMEM((band, units), bf16),
            pltpu.VMEM((ticks, n_dp, rows, units), f32),
            pltpu.VMEM((ticks, n_dp, rows, units), f32),
            pltpu.VMEM((ticks, band, units), bf16),
            pltpu.VMEM((band, units), bf16),
            pltpu.VMEM((band, units), bf16),
            pltpu.VMEM((ticks, band, units), bf16),
            pltpu.VMEM((band, width), bf16),
            pltpu.VMEM((ticks, 2, chips) + block, bf16),
            pltpu.VMEM((lanes, 2, chips) + block, bf16),
            pltpu.VMEM((lanes,) + block, bf16),
            pltpu.VMEM((lanes, 2, chips) + block, bf16),
            pltpu.VMEM((lanes, chips) + block, bf16),
            pltpu.VMEM((lanes, chips - 1) + block, bf16),
            pltpu.VMEM((lanes, chips - 1) + block, bf16),
            pltpu.SemaphoreType.DMA((4,)),
            pltpu.SemaphoreType.DMA((4 * ticks,)),
            pltpu.SemaphoreType.DMA((lanes, pieces, 2)),
            pltpu.SemaphoreType.DMA((lanes, pieces, 2, chips - 1)),
            pltpu.SemaphoreType.DMA((lanes, 2, chips)),
            pltpu.SemaphoreType.DMA((lanes, 2)),
            pltpu.SemaphoreType.DMA((ticks, 2, chips)),
            pltpu.SemaphoreType.DMA((ticks, 2)),
        ],
        compiler_params=pltpu.CompilerParams(
            collective_id=0, has_side_effects=True, vmem_limit_bytes=60 * 1024 * 1024
        ),
        name="relay",
    )(
        carry_act, carry_act_tan, carry_adj, carry_adj_tan, fresh_act, loss_cot, stash_act,
        stash_act_tan, norm_gain, up_weight, down_weight, up_dir, down_dir,
    )
    deep = band * ticks
    stash_sw = stash_out.reshape(deep, width)
    delta_sw = delta_out.reshape(deep, units)
    hidden_sw = hidden_out.reshape(deep, units)
    adj_flat = adj_out.reshape(deep, width)
    rows_shape = jax.ShapeDtypeStruct((1, rows, width), bf16)
    return tuple(
        pl.pallas_call(
            curvature_kernel,
            out_shape=(rows_shape,) * 4
            + (
                jax.ShapeDtypeStruct((1, width, units), bf16),
                jax.ShapeDtypeStruct((1, units, width), bf16),
            ),
            in_specs=[anywhere] * 5,
            out_specs=(anywhere,) * 6,
            scratch_shapes=[
                pltpu.VMEM((deep, width), bf16),
                pltpu.VMEM((deep, units), bf16),
                pltpu.VMEM((deep, units), bf16),
                pltpu.VMEM((deep, width), bf16),
                pltpu.VMEM((4, rows, width), bf16),
                pltpu.VMEM((width, units), bf16),
                pltpu.VMEM((units, width), bf16),
                pltpu.SemaphoreType.DMA((5,)),
                pltpu.SemaphoreType.DMA((4,)),
                pltpu.SemaphoreType.DMA((width // lane_chunk(width, 768),)),
                pltpu.SemaphoreType.DMA((units // lane_chunk(units, 384),)),
            ],
            compiler_params=pltpu.CompilerParams(vmem_limit_bytes=60 * 1024 * 1024),
            name="curvature",
        )(stash_sw, delta_sw, hidden_sw, adj_flat, final_out)
    )


def solution(mesh):
    in_specs = (
        P("section", "dp", None),
        P("section", "dp", None),
        P("section", "dp", None),
        P("section", "dp", None),
        P(None, "dp", None),
        P(None, "dp", None),
        P("section", None, "dp", None),
        P("section", None, "dp", None),
        P("section", None),
        P("section", None, "dp"),
        P("section", "dp", None),
        P("section", None, "dp"),
        P("section", "dp", None),
    )
    out_specs = (
        P("section", "dp", None),
        P("section", "dp", None),
        P("section", "dp", None),
        P("section", "dp", None),
        P("section", None, "dp"),
        P("section", "dp", None),
    )
    return jax.shard_map(shards, mesh=mesh, in_specs=in_specs, out_specs=out_specs, check_vma=False)
```
